256 devices in a mesh: vocab: 32 (over y, z), seq: 8 (over x, core).
Axes of the slice: x: 4, y: 4, z: 8, core: 2. Of those that a mesh axis runs over, the one named last changes fastest.
Arguments:
- hidden: bfloat16 [1024, 3584], P('seq', 'vocab'), may hold values from -16 to 16, as said below
- weight: bfloat16 [256000, 3584], P(('vocab', 'seq')), may hold values from -1 to 1, as said below
- targets: int32 [1024], P('seq'), may hold values from 0 to 255999
- loss_mask: int32 [1024], P('seq'), may hold values from 0 to 1, as said below
Outputs:
- lse: float32 [1024], P('seq')
- token_loss: float32 [1024], P('seq')
- ce_mean: float32 [], replicated
- z_root: float32 [], replicated
The draws below stay inside these ranges and needn't reach their ends.
Inputs may be any that keep to these rules, and one draw needn't show every extreme that they name: Each token's hidden state, of order one. `weight`: rows of order one over the square root of 3584. `loss_mask`: at least one token is counted.
All inputs are finite; a program needn't handle non-finite values.
Results may differ from the reference program's by a relative error of at most 0.0003.
Values may be sent and summed in bfloat16 or wider, within the bound.
No kernel may reach another device: no remote copies, remote signals or barrier semaphores. Data moves between devices by JAX's collectives and lax.ppermute only.
A program may use at most 64 MiB of HBM per device.

```python
import math
import jax
import jax.numpy as jnp
from jax import lax

D = 3584
VOC_DEV = 1000
VOCAB = 256000
TOKENS = 1024
N_SEQ = 8


def joint_draw(key):
    key_weight, key_hidden = jax.random.split(jax.random.fold_in(key, 7), 2)
    weight = jax.random.normal(key_weight, (VOCAB, D), jnp.float32) * (3.0 / math.sqrt(D))
    weight = jnp.clip(weight, -1.0, 1.0)
    hidden = jnp.clip(jax.random.normal(key_hidden, (TOKENS, D), jnp.float32), -6.0, 6.0)
    return (weight, hidden)


def draw_hidden(key, part):
    return joint_draw(key)[1].astype(jnp.bfloat16)


def draw_weight(key, part):
    return joint_draw(key)[0].astype(jnp.bfloat16)


def draw_loss_mask(key, part):
    key_bits, key_spot = jax.random.split(jax.random.fold_in(key, 11))
    position = jnp.arange(TOKENS, dtype=jnp.int32)
    bits = jax.random.randint(key_bits, (TOKENS,), 0, 1000)
    keep = (bits < 250 + 650 * position // TOKENS).astype(jnp.int32)
    spot = jax.random.randint(key_spot, (), 0, TOKENS)
    return keep.at[spot].set(1)


def set_ends(drawn, key, low, top_value):
    dims = drawn.shape
    spot = [jax.random.randint(jax.random.fold_in(key, axis), (), 0, dims[axis]) for axis in range(len(dims))]
    drawn = drawn.at[tuple(spot)].set(low)
    longest = dims.index(max(dims))
    spot[longest] = (spot[longest] + 1) % dims[longest]
    return drawn.at[tuple(spot)].set(top_value)


def setup_inputs(seed: int = 0) -> dict:
    key_of = jax.random.split(jax.random.key(seed), 5)
    hidden = draw_hidden(jax.random.fold_in(key_of[4], 71), 0)
    weight = draw_weight(jax.random.fold_in(key_of[4], 71), 0)
    targets = set_ends(jax.random.randint(key_of[2], (TOKENS,), 0, VOCAB), jax.random.fold_in(key_of[2], 1), 0, VOCAB - 1).astype(jnp.int32)
    loss_mask = draw_loss_mask(jax.random.fold_in(key_of[4], 71), 0)
    return {"hidden": hidden, "weight": weight, "targets": targets, "loss_mask": loss_mask}


def reference(hidden, weight, targets, loss_mask):
    block = VOC_DEV * N_SEQ
    count_blocks = VOCAB // block
    stacked = weight.reshape(count_blocks, block, D)
    indices = jnp.arange(count_blocks, dtype=jnp.int32)

    def step(carry, item):
        peak_now, total_now, target_now = carry
        weight_block, index = item
        logits = lax.dot_general(hidden, weight_block, (((1,), (1,)), ((), ())), preferred_element_type=jnp.float32)
        peak_next = jnp.maximum(peak_now, lax.optimization_barrier(jnp.max(logits, axis=1)))
        total_next = total_now * jnp.exp(peak_now - peak_next) + lax.optimization_barrier(jnp.sum(jnp.exp(logits - peak_next[:, None]), axis=1))
        columns = index * block + jnp.arange(block, dtype=jnp.int32)
        target_hit = columns[None, :] == targets[:, None]
        target_next = target_now + lax.optimization_barrier(jnp.sum(jnp.where(target_hit, logits, jnp.float32(0.0)), axis=1))
        return ((peak_next, total_next, target_next), None)
    start = (jnp.full((TOKENS,), -jnp.inf, jnp.float32), jnp.zeros((TOKENS,), jnp.float32), jnp.zeros((TOKENS,), jnp.float32))
    (row_peak, exp_total, target_logit), unused = lax.scan(step, start, (stacked, indices))
    lse = row_peak + jnp.log(exp_total)
    keep = loss_mask.astype(jnp.float32)
    token_loss = keep * (lse - target_logit)
    count = jnp.sum(loss_mask).astype(jnp.float32)
    ce_mean = jnp.sum(token_loss) / count
    z_root = jnp.sqrt(jnp.sum(keep * lse * lse) / count)
    return (lse, token_loss, ce_mean, z_root)
```

```python
import functools

import jax
import jax.numpy as jnp
from jax import lax
from jax.experimental import pallas as pl
from jax.experimental.pallas import tpu as pltpu
from jax.sharding import Mesh
from jax.sharding import PartitionSpec as P


OFFSETS = (0, 1, 3, 2)


def shifted(array, axis, offset):
    size = lax.axis_size(axis)
    return lax.ppermute(array, axis, [((k + offset) % size, k) for k in range(size)])


def around(array, axis):
    return [array] + [shifted(array, axis, offset) for offset in OFFSETS[1:]]


def from_everyone(array, axis):
    length = 1
    for name in axis if isinstance(axis, tuple) else (axis,):
        length *= lax.axis_size(name)
    return lax.all_to_all(
        jnp.broadcast_to(array[None], (length, *array.shape)), axis, 0, 0, tiled=True
    )


def head_kernel(place, ids, *refs):
    by_x, by_y = refs[0:4], refs[4:8]
    weights, out = refs[8:10], refs[10]
    gathered, held, logits, sems = refs[11:]
    copies = [
        pltpu.make_async_copy(weights[k], held.at[k], sems.at[k]) for k in range(2)
    ]
    for copy in copies:
        copy.start()
    half = by_x[0].shape[1]
    block = 2 * half
    for j in range(4):
        start = pl.multiple_of(place[j] * block, block)
        for i in range(4):
            lanes = slice(i * 128, (i + 1) * 128)
            gathered[pl.ds(start, half), lanes] = by_x[i][j]
            gathered[pl.ds(start + half, half), lanes] = by_y[j][i]
    rows = held.shape[1]
    found = {}
    for k in range(2):
        copies[k].wait()
        for side in range(2):
            lanes = slice(side * 256, (side + 1) * 256)
            logits[...] = jnp.dot(
                held[k], gathered[:, lanes], preferred_element_type=jnp.float32
            )
            peak = jnp.max(logits[...], axis=0, keepdims=True)
            total = jnp.sum(jnp.exp(logits[...] - peak), axis=0, keepdims=True)
            wanted = ids[:, lanes] - place[4 + k]
            row = lax.broadcasted_iota(jnp.int32, (rows, 256), 0)
            target = jnp.sum(
                jnp.where(row == wanted, logits[...], 0.0), axis=0, keepdims=True
            )
            found[k, side] = peak, total, target
    for side in range(2):
        (peak, total, target), (peak2, total2, target2) = found[0, side], found[1, side]
        top = jnp.maximum(peak, peak2)
        total = total * jnp.exp(peak - top) + total2 * jnp.exp(peak2 - top)
        lse = top + jnp.log(total)
        target = target + target2
        for i in range(2):
            at = place[6 + side * 2 + i]
            lanes = slice(i * 128, (i + 1) * 128)
            out[at, :, 0:128] = lse[:, lanes]
            out[at, :, 128:256] = target[:, lanes]


def combined(parts):
    lse, target = parts[..., :128], parts[..., 128:]
    top = jnp.max(lse, axis=0)
    lse = top + jnp.log(jnp.sum(jnp.exp(lse - top), axis=0))
    return jnp.concatenate([lse, jnp.sum(target, axis=0)], axis=-1)


def on_device(hidden, weight, targets, loss_mask):
    rows, depth = weight.shape
    tokens = targets.shape[0]
    x, y, z, c = (lax.axis_index(name) for name in ("x", "y", "z", "c"))
    other = lax.ppermute(weight, "c", [(0, 1), (1, 0)])
    ints = jnp.stack([targets, loss_mask])
    ints = jnp.stack(around(ints, "x"))
    ids = ints[:, 0].reshape(1, 4 * tokens)

    block = hidden.T
    mine = from_everyone(block, "z")
    n_z = mine.shape[0]
    first = mine[: n_z // 2].reshape(-1, tokens)
    second = mine[n_z // 2 :].reshape(-1, tokens)
    first, second = jnp.stack(around(first, "y")), jnp.stack(around(second, "x"))
    by_x, by_y = around(first, "x"), around(second, "y")

    index = ((y * n_z + z) * 4 + x) * 2 + c
    place = jnp.stack(
        [(y + offset) % 4 for offset in OFFSETS]
        + [index * rows, (index + 1 - 2 * c) * rows]
        + [(x + offset) % 4 for offset in OFFSETS]
    ).astype(jnp.int32)
    vmem = pl.BlockSpec(memory_space=pltpu.VMEM)
    found = pl.pallas_call(
        head_kernel,
        out_shape=jax.ShapeDtypeStruct((4, 1, 2 * tokens), jnp.float32),
        in_specs=[pl.BlockSpec(memory_space=pltpu.SMEM)]
        + [vmem] * 9
        + [pl.BlockSpec(memory_space=pl.ANY)] * 2,
        out_specs=vmem,
        scratch_shapes=[
            pltpu.VMEM((depth, 4 * tokens), jnp.bfloat16),
            pltpu.VMEM((2, rows, depth), jnp.bfloat16),
            pltpu.VMEM((rows, 256), jnp.float32),
            pltpu.SemaphoreType.DMA((2,)),
        ],
        compiler_params=pltpu.CompilerParams(vmem_limit_bytes=48 * 1024 * 1024),
        name="head",
    )(place, ids, *by_x, *by_y, weight, other)

    found = combined(from_everyone(found, ("y", "x")))
    found = combined(from_everyone(found, "z"))[:, 0]
    lse_all, target_all = found[:, :tokens], found[:, tokens:]
    keep = jnp.zeros((4, tokens), jnp.float32)
    for r, offset in enumerate(OFFSETS):
        keep = lax.dynamic_update_slice(
            keep, ints[r, 1:2].astype(jnp.float32), ((x + offset) % 4, 0)
        )
    loss_all = keep * (lse_all - target_all)
    sums = jnp.stack(
        [jnp.sum(loss_all), jnp.sum(keep * lse_all * lse_all), jnp.sum(keep)]
    )
    sums = sums + lax.ppermute(sums, "c", [(0, 1), (1, 0)])
    lse = lax.dynamic_slice_in_dim(lse_all, x, 1, 0)[0]
    token_loss = lax.dynamic_slice_in_dim(loss_all, x, 1, 0)[0]
    return (lse, token_loss, sums[0] / sums[2], jnp.sqrt(sums[1] / sums[2]))


def solution(mesh):
    split = Mesh(mesh.devices.reshape(4, 8, 4, 2), ("y", "z", "x", "c"))
    seq, vocab = ("x", "c"), ("y", "z")
    in_specs = (P(seq, vocab), P(vocab + seq, None), P(seq), P(seq))
    out_specs = (P(seq), P(seq), P(), P())
    return jax.shard_map(
        on_device, mesh=split, in_specs=in_specs, out_specs=out_specs, check_vma=False
    )
```

```python
import jax
import jax.numpy as jnp
from jax import lax
from jax.experimental import pallas as pl
from jax.experimental.pallas import tpu as pltpu
from jax.sharding import Mesh
from jax.sharding import PartitionSpec as P


OFFSETS = (0, 1, 3, 2)
LANES = 128
EXTRA = 16
VMEM = pl.BlockSpec(memory_space=pltpu.VMEM)
ANY = pl.BlockSpec(memory_space=pl.ANY)
SMEM = pl.BlockSpec(memory_space=pltpu.SMEM)
SWAP = [(0, 1), (1, 0)]


def shifted(array, axis, offset):
    size = lax.axis_size(axis)
    return lax.ppermute(array, axis, [((k + offset) % size, k) for k in range(size)])


def around(array, axis):
    return [array] + [shifted(array, axis, offset) for offset in OFFSETS[1:]]


def exchanged(array, axis):
    return lax.all_to_all(array, axis, 0, 0, tiled=True)


def load_kernel(own, other, out, sems):
    copies = [
        pltpu.make_async_copy(part, out.at[k], sems.at[k])
        for k, part in enumerate((own, other))
    ]
    for copy in copies:
        copy.start()
    for copy in copies:
        copy.wait()


def head_kernel(place, ints, *refs):
    by_x, by_y, (held, out, table, logits) = refs[:4], refs[4:8], refs[8:]
    half = by_x[0].shape[1]
    for j in range(4):
        start = pl.multiple_of(place[j] * 2 * half, 2 * half)
        for i in range(4):
            lanes = slice(i * LANES, (i + 1) * LANES)
            table[pl.ds(start, half), lanes] = by_x[i][j]
            table[pl.ds(start + half, half), lanes] = by_y[j][i]
    rows = held.shape[1]
    row = lax.broadcasted_iota(jnp.int32, (rows, 256), 0)
    found = {}
    for k in range(2):
        for side in range(2):
            lanes = slice(side * 256, (side + 1) * 256)
            logits[k, side] = jnp.dot(
                held[k], table[:, lanes], preferred_element_type=jnp.float32
            )
            peak = jnp.max(logits[k, side], axis=0, keepdims=True)
            total = jnp.sum(jnp.exp(logits[k, side] - peak), axis=0, keepdims=True)
            digits = [
                jnp.concatenate(
                    [ints[2 * side + h, d : d + 1] for h in range(2)], axis=1
                ).astype(jnp.int32)
                for d in range(3)
            ]
            wanted = digits[0] + 256 * digits[1] + 65536 * digits[2] - place[4 + k]
            target = jnp.sum(
                jnp.where(row == wanted, logits[k, side], 0.0), axis=0, keepdims=True
            )
            found[k, side] = peak, total, target
    message = jnp.zeros((8, LANES), jnp.float32)
    line = lax.broadcasted_iota(jnp.int32, (8, LANES), 0)
    for side in range(2):
        (peak, total, target), (peak2, total2, target2) = found[0, side], found[1, side]
        top = jnp.maximum(peak, peak2)
        total = total * jnp.exp(peak - top) + total2 * jnp.exp(peak2 - top)
        lse = top + jnp.log(total)
        target = target + target2
        for i in range(2):
            at = place[6 + side * 2 + i]
            lanes = slice(i * LANES, (i + 1) * LANES)
            message = jnp.where(line == at, lse[:, lanes], message)
            message = jnp.where(line == 4 + at, target[:, lanes], message)
    for k in range(out.shape[0]):
        out[k] = message


def spread_kernel(block, out):
    for k in range(out.shape[0]):
        out[k] = block[...]


def joined(parts):
    top, summed = parts[0], parts[0]
    for part in parts[1:]:
        top, summed = jnp.maximum(top, part), summed + part
    total = jnp.exp(parts[0] - top)
    for part in parts[1:]:
        total = total + jnp.exp(part - top)
    line = lax.broadcasted_iota(jnp.int32, summed.shape, 0)
    return jnp.where(line < 4, top + jnp.log(total), summed)


def join_kernel(parts, out):
    message = joined([parts[k] for k in range(parts.shape[0])])
    for k in range(out.shape[0]):
        out[k] = message


def last_kernel(place, ints, parts, lse_out, loss_out, mean_out, root_out):
    line = lax.broadcasted_iota(jnp.int32, (4, LANES), 0)
    sums, rows = [], []
    for c in range(2):
        message = joined([parts[k] for k in range(c, parts.shape[0], 2)])
        lse, target = message[:4], message[4:]
        keep = jnp.zeros((4, LANES), jnp.float32)
        for i in range(4):
            own = ints[i, 3:4].astype(jnp.float32)
            their = ints[i, 4:5].astype(jnp.float32)
            picked = jnp.where(place[10] == c, own, their)
            keep = jnp.where(line == place[6 + i], picked, keep)
        loss = keep * (lse - target)
        rows.append((lse, loss))
        sums.append((loss, keep * lse * lse, keep))
    for out, first, second in zip((lse_out, loss_out), *rows):
        both = jnp.where(place[10] == 0, first, second)
        out[...] = jnp.sum(
            jnp.where(line == place[6], both, 0.0), axis=0, keepdims=True
        )
    loss, square, count = (
        jnp.sum(first + second, keepdims=True) for first, second in zip(*sums)
    )
    mean_out[...] = loss / count
    root_out[...] = jnp.sqrt(square / count)


def call(kernel, name, inputs, specs, out_shape, scratch=(), limit=8):
    single = not isinstance(out_shape, tuple)
    return pl.pallas_call(
        kernel,
        out_shape=out_shape,
        in_specs=specs,
        out_specs=VMEM if single else tuple(VMEM for _ in out_shape),
        scratch_shapes=list(scratch),
        compiler_params=pltpu.CompilerParams(vmem_limit_bytes=limit * 1024 * 1024),
        name=name,
    )(*inputs)


def on_device(hidden, weight, targets, loss_mask):
    rows = weight.shape[0]
    x, y, z, c = (lax.axis_index(name) for name in ("x", "y", "z", "c"))
    n_z = lax.axis_size("z")
    other = lax.ppermute(weight, "c", SWAP)
    their_mask = lax.ppermute(loss_mask, "c", SWAP)
    ints = jnp.stack(
        [targets % 256, targets // 256 % 256, targets // 65536, loss_mask, their_mask]
    )
    ints = jnp.pad(ints, ((0, EXTRA - 5), (0, 0))).astype(jnp.bfloat16)

    block = hidden.T
    mine = call(
        spread_kernel,
        "spread",
        (block,),
        [VMEM],
        pltpu.VMEM((n_z, *block.shape), block.dtype),
    )
    mine = exchanged(mine, "z")
    first = mine[: n_z // 2].reshape(-1, LANES)
    second = mine[n_z // 2 :].reshape(-1, LANES)
    half = first.shape[0]
    second = jnp.concatenate([second, ints])
    first, second = lax.optimization_barrier((around(first, "y"), around(second, "x")))
    ints = jnp.stack([part[half:] for part in second])
    first = jnp.stack(first)
    second = jnp.stack([part[:half] for part in second])
    by_x, by_y = around(first, "x"), around(second, "y")

    index = ((y * n_z + z) * 4 + x) * 2 + c
    place = jnp.stack(
        [(y + offset) % 4 for offset in OFFSETS]
        + [index * rows, (index + 1 - 2 * c) * rows]
        + [(x + offset) % 4 for offset in OFFSETS]
        + [c]
    ).astype(jnp.int32)
    held = call(
        load_kernel,
        "load",
        (weight, other),
        [ANY] * 2,
        pltpu.VMEM((2, *weight.shape), weight.dtype),
        [pltpu.SemaphoreType.DMA((2,))],
    )
    message = call(
        head_kernel,
        "head",
        (place, ints, *by_x, *by_y, held),
        [SMEM] + [VMEM] * 10,
        jax.ShapeDtypeStruct((16, 8, LANES), jnp.float32),
        [
            pltpu.VMEM((weight.shape[1], 512), jnp.bfloat16),
            pltpu.VMEM((2, 2, rows, 256), jnp.float32),
        ],
        24,
    )
    message = call(
        join_kernel,
        "join",
        (exchanged(message, ("y", "x")),),
        [VMEM],
        jax.ShapeDtypeStruct((2 * n_z, 8, LANES), jnp.float32),
    )
    line = jax.ShapeDtypeStruct((1, LANES), jnp.float32)
    one = jax.ShapeDtypeStruct((1, 1), jnp.float32)
    lse, loss, mean, root = call(
        last_kernel,
        "last",
        (place, ints, exchanged(message, ("z", "c"))),
        [SMEM, VMEM, VMEM],
        (line, line, one, one),
    )
    return (lse[0], loss[0], mean[0, 0], root[0, 0])


def solution(mesh):
    split = Mesh(mesh.devices.reshape(4, 8, 4, 2), ("y", "z", "x", "c"))
    seq, vocab = ("x", "c"), ("y", "z")
    in_specs = (P(seq, vocab), P(vocab + seq, None), P(seq), P(seq))
    out_specs = (P(seq), P(seq), P(), P())
    return jax.shard_map(
        on_device, mesh=split, in_specs=in_specs, out_specs=out_specs, check_vma=False
    )
```

```python
import jax
import jax.numpy as jnp
from jax import lax
from jax.experimental import pallas as pl
from jax.experimental.pallas import tpu as pltpu
from jax.sharding import Mesh
from jax.sharding import PartitionSpec as P


OFFSETS = (0, 1, 3, 2)
LANES = 128
EXTRA = 16
MASKED = 1e30
VMEM = pl.BlockSpec(memory_space=pltpu.VMEM)
HBM = pl.BlockSpec(memory_space=pltpu.HBM)
SMEM = pl.BlockSpec(memory_space=pltpu.SMEM)
SWAP = [(0, 1), (1, 0)]


def shifted(array, axis, offset):
    size = lax.axis_size(axis)
    return lax.ppermute(array, axis, [((k + offset) % size, k) for k in range(size)])


def around(array, axis):
    return [array] + [shifted(array, axis, offset) for offset in OFFSETS[1:]]


def relayed(array, axis):
    half = array.shape[0] // 2
    up = shifted(array, axis, 1)
    down = shifted(array, axis, 3)
    low, high = shifted(up[:half], axis, 1), shifted(down[half:], axis, 3)
    return [array, up, down, low, high]


def exchanged(array, axis):
    return lax.all_to_all(array, axis, 0, 0, tiled=True)


def load_kernel(first, second, out, sems):
    copies = [
        pltpu.make_async_copy(part, out.at[k], sems.at[k])
        for k, part in enumerate((first, second))
    ]
    for copy in copies:
        copy.start()
    for copy in copies:
        copy.wait()


def half_depth(held, k, second, half):
    return jnp.concatenate(
        [
            held[k, :, (2 * j + second) * half : (2 * j + second + 1) * half]
            for j in range(4)
        ],
        axis=1,
    )


def set_rows(table, place, j, lanes, rows):
    half = rows.shape[0]
    table[pl.ds(pl.multiple_of(place[j] * half, half), half), lanes] = rows


def near_kernel(place, x0, x1, held, out, table):
    for j in range(4):
        for i, block in enumerate((x0, x1)):
            lanes = slice(i * LANES, (i + 1) * LANES)
            set_rows(table, place, j, lanes, block[j])
    for k in range(2):
        out[k] = jnp.dot(
            half_depth(held, k, 0, x0.shape[1]),
            table[...],
            preferred_element_type=jnp.float32,
        )


def far_kernel(place, x2, x3, x4, held, out, table):
    for j in range(4):
        set_rows(table, place, j, slice(0, LANES), x2[j])
        far = x3[j] if j < 2 else x4[j - 2]
        set_rows(table, place, j, slice(LANES, 2 * LANES), far)
    for k in range(2):
        out[k] = jnp.dot(
            half_depth(held, k, 0, x2.shape[1]),
            table[...],
            preferred_element_type=jnp.float32,
        )


def head_kernel(
    place, ints, y0, y1, y2, y3, y4, held, near, far, out, table, logits
):
    half = y0.shape[1]
    for i in range(4):
        lanes = slice(i * LANES, (i + 1) * LANES)
        for j, block in enumerate((y0, y1, y2)):
            set_rows(table, place, j, lanes, block[i])
        set_rows(table, place, 3, lanes, y3[i] if i < 2 else y4[i - 2])
    rows = held.shape[1]
    row = lax.broadcasted_iota(jnp.int32, (rows, 256), 0)
    found = {}
    for k in range(2):
        for side in range(2):
            lanes = slice(side * 256, (side + 1) * 256)
            logits[k, side] = (far if side else near)[k] + jnp.dot(
                half_depth(held, k, 1, half),
                table[:, lanes],
                preferred_element_type=jnp.float32,
            )
            peak = jnp.max(logits[k, side], axis=0, keepdims=True)
            total = jnp.sum(jnp.exp(logits[k, side] - peak), axis=0, keepdims=True)
            digits = [
                jnp.concatenate(
                    [ints[2 * side + h, d : d + 1] for h in range(2)], axis=1
                ).astype(jnp.int32)
                for d in range(3)
            ]
            kept = jnp.concatenate(
                [ints[2 * side + h, 3:4] for h in range(2)], axis=1
            ).astype(jnp.float32)
            wanted = digits[0] + 256 * digits[1] + 65536 * digits[2] - place[4 + k]
            target = jnp.sum(
                jnp.where(row == wanted, logits[k, side], 0.0), axis=0, keepdims=True
            )
            found[k, side] = peak, total, jnp.where(kept > 0.5, target, MASKED)
    message = jnp.zeros((8, LANES), jnp.float32)
    line = lax.broadcasted_iota(jnp.int32, (8, LANES), 0)
    for side in range(2):
        (peak, total, target), (peak2, total2, target2) = found[0, side], found[1, side]
        top = jnp.maximum(peak, peak2)
        total = total * jnp.exp(peak - top) + total2 * jnp.exp(peak2 - top)
        lse = top + jnp.log(total)
        target = target + target2
        for i in range(2):
            at = place[6 + side * 2 + i]
            lanes = slice(i * LANES, (i + 1) * LANES)
            message = jnp.where(line == at, lse[:, lanes], message)
            message = jnp.where(line == 4 + at, target[:, lanes], message)
    for k in range(out.shape[0]):
        out[k] = message


def spread_kernel(block, out):
    for k in range(out.shape[0]):
        out[k] = block[...]


def digits_kernel(targets, mask, out):
    line = lax.broadcasted_iota(jnp.int32, out.shape, 0)
    ids = targets[...]
    both = jnp.zeros(out.shape, jnp.float32)
    for k, row in enumerate([ids & 255, (ids >> 8) & 255, ids >> 16, mask[...]]):
        both = jnp.where(line == k, row.astype(jnp.float32), both)
    out[...] = both.astype(out.dtype)


def joined(parts):
    top, summed = parts[0], parts[0]
    for part in parts[1:]:
        top, summed = jnp.maximum(top, part), summed + part
    total = jnp.exp(parts[0] - top)
    for part in parts[1:]:
        total = total + jnp.exp(part - top)
    line = lax.broadcasted_iota(jnp.int32, summed.shape, 0)
    return jnp.where(line < 4, top + jnp.log(total), summed)


def join_kernel(parts, out):
    message = joined([parts[k] for k in range(parts.shape[0])])
    for k in range(out.shape[0]):
        out[k] = message


def last_kernel(place, parts, lse_out, loss_out, mean_out, root_out):
    line = lax.broadcasted_iota(jnp.int32, (4, LANES), 0)
    sums, rows = [], []
    for c in range(2):
        message = joined([parts[k] for k in range(c, parts.shape[0], 2)])
        lse, target = message[:4], message[4:]
        kept = target < 0.5 * MASKED
        loss = jnp.where(kept, lse - target, 0.0)
        rows.append((lse, loss))
        sums.append((loss, jnp.where(kept, lse * lse, 0.0), jnp.where(kept, 1.0, 0.0)))
    for out, first, second in zip((lse_out, loss_out), *rows):
        both = jnp.where(place[10] == 0, first, second)
        out[...] = jnp.sum(
            jnp.where(line == place[6], both, 0.0), axis=0, keepdims=True
        )
    loss, square, count = (
        jnp.sum(first + second, keepdims=True) for first, second in zip(*sums)
    )
    mean_out[...] = loss / count
    root_out[...] = jnp.sqrt(square / count)


def call(kernel, inputs, specs, out_shape, scratch=(), limit=8):
    single = not isinstance(out_shape, tuple)
    return pl.pallas_call(
        kernel,
        out_shape=out_shape,
        in_specs=specs,
        out_specs=VMEM if single else tuple(VMEM for _ in out_shape),
        scratch_shapes=list(scratch),
        compiler_params=pltpu.CompilerParams(vmem_limit_bytes=limit * 1024 * 1024),
    )(*inputs)


def on_device(hidden, weight, targets, loss_mask):
    rows = weight.shape[0]
    x, y, z, c = (lax.axis_index(name) for name in ("x", "y", "z", "c"))
    n_z = lax.axis_size("z")
    other = lax.ppermute(weight, "c", SWAP)
    block = hidden.T
    ints = call(
        digits_kernel,
        (targets[None], loss_mask[None]),
        [VMEM] * 2,
        jax.ShapeDtypeStruct((EXTRA, LANES), block.dtype),
    )
    mine = call(
        spread_kernel,
        (block,),
        [VMEM],
        jax.ShapeDtypeStruct((n_z, *block.shape), block.dtype),
    )
    mine = exchanged(mine, "z")
    first = mine[: n_z // 2].reshape(-1, LANES)
    second = mine[n_z // 2 :].reshape(-1, LANES)
    half = first.shape[0]
    second = jnp.concatenate([second, ints])
    second, first = around(second, "x"), around(first, "y")
    ints = jnp.stack([part[half:] for part in second])
    first = jnp.stack(first)
    second = jnp.stack([part[:half] for part in second])
    held = call(
        load_kernel,
        [pltpu.with_memory_space_constraint(w, pltpu.HBM) for w in (weight, other)],
        [HBM] * 2,
        pltpu.VMEM((2, *weight.shape), weight.dtype),
        [pltpu.SemaphoreType.DMA((2,))],
    )
    by_x, by_y = relayed(first, "x"), relayed(second, "y")

    index = ((y * n_z + z) * 4 + x) * 2 + c
    place = jnp.stack(
        [(y + offset) % 4 for offset in OFFSETS]
        + [index * rows, (index + 1 - 2 * c) * rows]
        + [(x + offset) % 4 for offset in OFFSETS]
        + [c]
    ).astype(jnp.int32)
    depth = weight.shape[1] // 2
    near, far = (
        call(
            kernel,
            (place, *blocks, held),
            [SMEM] + [VMEM] * (len(blocks) + 1),
            pltpu.VMEM((2, rows, 256), jnp.float32),
            [pltpu.VMEM((depth, 256), jnp.bfloat16)],
            24,
        )
        for kernel, blocks in ((near_kernel, by_x[:2]), (far_kernel, by_x[2:]))
    )
    message = call(
        head_kernel,
        (place, ints, *by_y, held, near, far),
        [SMEM] + [VMEM] * 9,
        jax.ShapeDtypeStruct((16, 8, LANES), jnp.float32),
        [
            pltpu.VMEM((depth, 512), jnp.bfloat16),
            pltpu.VMEM((2, 2, rows, 256), jnp.float32),
        ],
        24,
    )
    message = call(
        join_kernel,
        (exchanged(message, ("y", "x")),),
        [VMEM],
        jax.ShapeDtypeStruct((2 * n_z, 8, LANES), jnp.float32),
    )
    line = jax.ShapeDtypeStruct((1, LANES), jnp.float32)
    one = jax.ShapeDtypeStruct((1, 1), jnp.float32)
    lse, loss, mean, root = call(
        last_kernel,
        (place, exchanged(message, ("z", "c"))),
        [SMEM, VMEM],
        (line, line, one, one),
    )
    return (lse[0], loss[0], mean[0, 0], root[0, 0])


def solution(mesh):
    split = Mesh(mesh.devices.reshape(4, 8, 4, 2), ("y", "z", "x", "c"))
    seq, vocab = ("x", "c"), ("y", "z")
    in_specs = (P(seq, vocab), P(vocab + seq, None), P(seq), P(seq))
    out_specs = (P(seq), P(seq), P(), P())

    return jax.shard_map(
        on_device, mesh=split, in_specs=in_specs, out_specs=out_specs, check_vma=False
    )
```

```python
import jax
import jax.numpy as jnp
from jax import lax
from jax.experimental import pallas as pl
from jax.experimental.pallas import tpu as pltpu
from jax.sharding import Mesh
from jax.sharding import PartitionSpec as P


OFFSETS = (0, 1, 3, 2)
LANES = 128
EXTRA = 16
MASKED = 1e30
VMEM = pl.BlockSpec(memory_space=pltpu.VMEM)
HBM = pl.BlockSpec(memory_space=pltpu.HBM)
SMEM = pl.BlockSpec(memory_space=pltpu.SMEM)
SWAP = [(0, 1), (1, 0)]


def shifted(array, axis, offset):
    size = lax.axis_size(axis)
    return lax.ppermute(array, axis, [((k + offset) % size, k) for k in range(size)])


def around(array, axis):
    return [array] + [shifted(array, axis, offset) for offset in OFFSETS[1:]]


def relayed(array, axis):
    half = array.shape[0] // 2
    up = shifted(array, axis, 1)
    down = shifted(array, axis, 3)
    low, high = shifted(up[:half], axis, 1), shifted(down[half:], axis, 3)
    return [array, up, down, low, high]


def exchanged(array, axis):
    return lax.all_to_all(array, axis, 0, 0, tiled=True)


def load_kernel(first, second, out, sems):
    chunk = first.shape[0] // sems.shape[1]
    copies = [
        pltpu.make_async_copy(
            part.at[pl.ds(n * chunk, chunk)],
            out.at[k, pl.ds(n * chunk, chunk)],
            sems.at[k, n],
        )
        for n in range(sems.shape[1])
        for k, part in enumerate((first, second))
    ]
    for copy in copies:
        copy.start()
    for copy in copies:
        copy.wait()


def half_depth(held, k, second, half):
    return jnp.concatenate(
        [
            held[k, :, (2 * j + second) * half : (2 * j + second + 1) * half]
            for j in range(4)
        ],
        axis=1,
    )


def set_rows(table, place, j, lanes, rows):
    half = rows.shape[0]
    table[pl.ds(pl.multiple_of(place[j] * half, half), half), lanes] = rows


def near_kernel(place, x0, x1, held, out, table):
    for j in range(4):
        for i, block in enumerate((x0, x1)):
            lanes = slice(i * LANES, (i + 1) * LANES)
            set_rows(table, place, j, lanes, block[j])
    for k in range(2):
        out[k] = jnp.dot(
            half_depth(held, k, 0, x0.shape[1]),
            table[...],
            preferred_element_type=jnp.float32,
        )


def far_kernel(place, x2, x3, x4, held, out, table):
    for j in range(4):
        set_rows(table, place, j, slice(0, LANES), x2[j])
        far = x3[j] if j < 2 else x4[j - 2]
        set_rows(table, place, j, slice(LANES, 2 * LANES), far)
    for k in range(2):
        out[k] = jnp.dot(
            half_depth(held, k, 0, x2.shape[1]),
            table[...],
            preferred_element_type=jnp.float32,
        )


def head_kernel(
    place, ints, y0, y1, y2, y3, y4, held, near, far, out, table, logits
):
    half = y0.shape[1]
    for i in range(4):
        lanes = slice(i * LANES, (i + 1) * LANES)
        for j, block in enumerate((y0, y1, y2)):
            set_rows(table, place, j, lanes, block[i])
        set_rows(table, place, 3, lanes, y3[i] if i < 2 else y4[i - 2])
    rows = held.shape[1]
    row = lax.broadcasted_iota(jnp.int32, (rows, 256), 0)
    found = {}
    for k in range(2):
        for side in range(2):
            lanes = slice(side * 256, (side + 1) * 256)
            logits[k, side] = (far if side else near)[k] + jnp.dot(
                half_depth(held, k, 1, half),
                table[:, lanes],
                preferred_element_type=jnp.float32,
            )
            peak = jnp.max(logits[k, side], axis=0, keepdims=True)
            total = jnp.sum(jnp.exp(logits[k, side] - peak), axis=0, keepdims=True)
            digits = [
                jnp.concatenate(
                    [ints[2 * side + h, d : d + 1] for h in range(2)], axis=1
                ).astype(jnp.int32)
                for d in range(3)
            ]
            kept = jnp.concatenate(
                [ints[2 * side + h, 3:4] for h in range(2)], axis=1
            ).astype(jnp.float32)
            wanted = digits[0] + 256 * digits[1] + 65536 * digits[2] - place[4 + k]
            target = jnp.sum(
                jnp.where(row == wanted, logits[k, side], 0.0), axis=0, keepdims=True
            )
            found[k, side] = peak, total, jnp.where(kept > 0.5, target, MASKED)
    message = jnp.zeros((8, LANES), jnp.float32)
    line = lax.broadcasted_iota(jnp.int32, (8, LANES), 0)
    for side in range(2):
        (peak, total, target), (peak2, total2, target2) = found[0, side], found[1, side]
        top = jnp.maximum(peak, peak2)
        total = total * jnp.exp(peak - top) + total2 * jnp.exp(peak2 - top)
        lse = top + jnp.log(total)
        target = target + target2
        for i in range(2):
            at = place[6 + side * 2 + i]
            lanes = slice(i * LANES, (i + 1) * LANES)
            message = jnp.where(line == at, lse[:, lanes], message)
            message = jnp.where(line == 4 + at, target[:, lanes], message)
    for k in range(out.shape[0]):
        out[k] = message


def spread_kernel(block, out):
    for k in range(out.shape[0]):
        out[k] = block[...]


def digits_kernel(targets, mask, out):
    line = lax.broadcasted_iota(jnp.int32, out.shape, 0)
    ids = targets[...]
    both = jnp.zeros(out.shape, jnp.float32)
    for k, row in enumerate([ids & 255, (ids >> 8) & 255, ids >> 16, mask[...]]):
        both = jnp.where(line == k, row.astype(jnp.float32), both)
    out[...] = both.astype(out.dtype)


def joined(parts):
    top, summed = parts[0], parts[0]
    for part in parts[1:]:
        top, summed = jnp.maximum(top, part), summed + part
    total = jnp.exp(parts[0] - top)
    for part in parts[1:]:
        total = total + jnp.exp(part - top)
    line = lax.broadcasted_iota(jnp.int32, summed.shape, 0)
    return jnp.where(line < 4, top + jnp.log(total), summed)


def join_kernel(parts, out):
    message = joined([parts[k] for k in range(parts.shape[0])])
    for k in range(out.shape[0]):
        out[k] = message


def last_kernel(place, parts, lse_out, loss_out, mean_out, root_out):
    line = lax.broadcasted_iota(jnp.int32, (4, LANES), 0)
    sums, rows = [], []
    for c in range(2):
        message = joined([parts[k] for k in range(c, parts.shape[0], 2)])
        lse, target = message[:4], message[4:]
        kept = target < 0.5 * MASKED
        loss = jnp.where(kept, lse - target, 0.0)
        rows.append((lse, loss))
        sums.append((loss, jnp.where(kept, lse * lse, 0.0), jnp.where(kept, 1.0, 0.0)))
    for out, first, second in zip((lse_out, loss_out), *rows):
        both = jnp.where(place[10] == 0, first, second)
        out[...] = jnp.sum(
            jnp.where(line == place[6], both, 0.0), axis=0, keepdims=True
        )
    loss, square, count = (
        jnp.sum(first + second, keepdims=True) for first, second in zip(*sums)
    )
    mean_out[...] = loss / count
    root_out[...] = jnp.sqrt(square / count)


def call(kernel, inputs, specs, out_shape, scratch=(), limit=8):
    single = not isinstance(out_shape, tuple)
    return pl.pallas_call(
        kernel,
        out_shape=out_shape,
        in_specs=specs,
        out_specs=VMEM if single else tuple(VMEM for _ in out_shape),
        scratch_shapes=list(scratch),
        compiler_params=pltpu.CompilerParams(vmem_limit_bytes=limit * 1024 * 1024),
    )(*inputs)


def on_device(hidden, weight, targets, loss_mask):
    rows = weight.shape[0]
    x, y, z, c = (lax.axis_index(name) for name in ("x", "y", "z", "c"))
    n_z = lax.axis_size("z")
    other = lax.ppermute(weight, "c", SWAP)
    block = hidden.T
    ints = call(
        digits_kernel,
        (targets[None], loss_mask[None]),
        [VMEM] * 2,
        jax.ShapeDtypeStruct((EXTRA, LANES), block.dtype),
    )
    mine = call(
        spread_kernel,
        (block,),
        [VMEM],
        jax.ShapeDtypeStruct((n_z, *block.shape), block.dtype),
    )
    mine = exchanged(mine, "z")
    first = mine[: n_z // 2].reshape(-1, LANES)
    second = mine[n_z // 2 :].reshape(-1, LANES)
    half = first.shape[0]
    second = jnp.concatenate([second, ints])
    second, first = around(second, "x"), around(first, "y")
    ints = jnp.stack([part[half:] for part in second])
    first = jnp.stack(first)
    second = jnp.stack([part[:half] for part in second])
    held = call(
        load_kernel,
        [pltpu.with_memory_space_constraint(w, pltpu.HBM) for w in (weight, other)],
        [HBM] * 2,
        pltpu.VMEM((2, *weight.shape), weight.dtype),
        [pltpu.SemaphoreType.DMA((2, 5))],
    )
    by_x, by_y = relayed(first, "x"), relayed(second, "y")

    index = ((y * n_z + z) * 4 + x) * 2 + c
    place = jnp.stack(
        [(y + offset) % 4 for offset in OFFSETS]
        + [index * rows, (index + 1 - 2 * c) * rows]
        + [(x + offset) % 4 for offset in OFFSETS]
        + [c]
    ).astype(jnp.int32)
    depth = weight.shape[1] // 2
    near, far = (
        call(
            kernel,
            (place, *blocks, held),
            [SMEM] + [VMEM] * (len(blocks) + 1),
            pltpu.VMEM((2, rows, 256), jnp.float32),
            [pltpu.VMEM((depth, 256), jnp.bfloat16)],
            24,
        )
        for kernel, blocks in ((near_kernel, by_x[:2]), (far_kernel, by_x[2:]))
    )
    message = call(
        head_kernel,
        (place, ints, *by_y, held, near, far),
        [SMEM] + [VMEM] * 9,
        jax.ShapeDtypeStruct((16, 8, LANES), jnp.float32),
        [
            pltpu.VMEM((depth, 512), jnp.bfloat16),
            pltpu.VMEM((2, 2, rows, 256), jnp.float32),
        ],
        24,
    )
    message = call(
        join_kernel,
        (exchanged(message, ("y", "x")),),
        [VMEM],
        jax.ShapeDtypeStruct((2 * n_z, 8, LANES), jnp.float32),
    )
    line = jax.ShapeDtypeStruct((1, LANES), jnp.float32)
    one = jax.ShapeDtypeStruct((1, 1), jnp.float32)
    lse, loss, mean, root = call(
        last_kernel,
        (place, exchanged(message, ("z", "c"))),
        [SMEM, VMEM],
        (line, line, one, one),
    )
    return (lse[0], loss[0], mean[0, 0], root[0, 0])


def solution(mesh):
    split = Mesh(mesh.devices.reshape(4, 8, 4, 2), ("y", "z", "x", "c"))
    seq, vocab = ("x", "c"), ("y", "z")
    in_specs = (P(seq, vocab), P(vocab + seq, None), P(seq), P(seq))
    out_specs = (P(seq), P(seq), P(), P())

    return jax.shard_map(
        on_device, mesh=split, in_specs=in_specs, out_specs=out_specs, check_vma=False
    )
```
